32 devices in a mesh: gx: 4 (over y, core), gy: 8 (over z, x).
Axes of the slice: x: 2, y: 2, z: 4, core: 2. Of those that a mesh axis runs over, the one named last changes fastest.
Arguments:
- disp: float32 [3, 32, 128, 128], P(None, 'gx', 'gy'), may hold values from -3 to 3
- vel: float32 [3, 32, 128, 128], P(None, 'gx', 'gy'), may hold values from -30 to 30
- load: float32 [3, 32, 128, 128], P(None, 'gx', 'gy'), may hold values from -96 to 96
- flags: int32 [32, 128, 128], P('gx', 'gy'), may hold values 0 or 1
- mask_bits: int32 [4, 32, 128, 128], P(None, 'gx', 'gy'), may hold values from 0 to 2147483647, as said below
Outputs:
- disp_out: float32 [3, 32, 128, 128], P(None, 'gx', 'gy')
- vel_out: float32 [3, 32, 128, 128], P(None, 'gx', 'gy')
The draws below stay inside these ranges and needn't reach their ends.
Inputs may be any that keep to these rules, and one draw needn't show every extreme that they name: `mask_bits`: bit b (0 to 30) of word w marks the cell's bond to neighbour number 31 w + b as broken; bit 31, and bits of numbers 122 and above, are zero.
All inputs are finite; a program needn't handle non-finite values. No bound on the sum of `flags` on one device may be relied on, other than what follows from the above.
Results may differ from the reference program's by a relative error of at most 0.0001.
Values sent between devices are 32-bit elements; how exact they have to be, the bound alone decides.
A program may use at most 128 MiB of HBM per device.

```python
import math
import jax
import jax.numpy as jnp
from jax import lax

NZ = 128
ITERS = 8
NX = 32
NY = 128


def neighbour_table_drawn():
    table = []
    for across in range(-3, 4):
        for along in range(-3, 4):
            for upward in range(-3, 4):
                length = across * across + along * along + upward * upward
                if 0 < length <= 9:
                    table.append((across, along, upward))
    return table


def draw_vel(key, part):
    places_x = jnp.arange(NX, dtype=jnp.float32) / max(NX - 1, 1)
    places_y = jnp.arange(NY, dtype=jnp.float32) / max(NY - 1, 1)
    amplitude = 0.3 * (1.0 + 2.0 * places_x)[:, None, None] * (1.0 + 2.0 * places_y)[None, :, None]
    first = jax.random.fold_in(key, 11)
    base = jnp.clip(jax.random.normal(first, (3, NX, NY, NZ), jnp.float32), -4.0, 4.0)
    return (amplitude[None] * base).astype(jnp.float32)


def draw_mask_bits(key, part):
    table = neighbour_table_drawn()
    places_x = jnp.arange(NX, dtype=jnp.int32)[:, None, None]
    places_y = jnp.arange(NY, dtype=jnp.int32)[None, :, None]
    middle = NX // 2
    words = []
    for word in range(4):
        packed = jnp.zeros((NX, NY, NZ), jnp.int32)
        for bit in range(31):
            number = 31 * word + bit
            if number < 122:
                across = table[number][0]
                coin = jax.random.randint(jax.random.fold_in(key, 100 + number), (NX, NY, NZ), 0, 16)
                crosses = (places_x < middle) & (places_x + across >= middle) | (places_x >= middle) & (places_x + across < middle)
                crack = crosses & (places_y < NY // 2)
                broken = (coin == 0) | crack
                packed = packed | broken.astype(jnp.int32) << bit
        words.append(packed)
    return jnp.stack(words)


def set_ends(array, rng, low, high):
    index_at = [jax.random.randint(jax.random.fold_in(rng, axis), (), 0, length) for axis, length in enumerate(array.shape)]
    widest = array.shape.index(max(array.shape))
    next_to = index_at[:widest] + [(index_at[widest] + 1) % array.shape[widest]] + index_at[widest + 1:]
    return array.at[tuple(index_at)].set(low).at[tuple(next_to)].set(high)


def level_of(rng, dims, split, low, high):
    factor_of = 1.0
    for dim, shards_of in split:
        steps = jax.random.uniform(jax.random.fold_in(jax.random.fold_in(rng, 6), dim), (shards_of,), jnp.float32, low / len(split), high / len(split))
        factor_of = factor_of * jnp.repeat(jnp.exp(steps), dims[dim] // shards_of).reshape((-1,) + (1,) * (len(dims) - 1 - dim))
    return factor_of


def scatter_about(own_key, dims, spread, bound, split=(), kind=jnp.bfloat16):
    factor_of = level_of(own_key, dims, split, -0.22, 0.18) if split else 1.0
    entries = jax.random.normal(own_key, dims, jnp.float32) * spread * factor_of
    return jnp.minimum(jnp.maximum(entries, -bound), bound).astype(kind)


def setup_inputs(seed: int = 0) -> dict:
    key_of = jax.random.split(jax.random.key(seed), 6)
    return {
        "disp": scatter_about(key_of[0], (3, NX, NY, NZ), 0.5, 3.0, ((1, 4), (2, 8)), jnp.float32),
        "vel": draw_vel(jax.random.fold_in(key_of[5], 71), 0),
        "load": scatter_about(key_of[2], (3, NX, NY, NZ), 16.0, 96.0, ((1, 4), (2, 8)), jnp.float32),
        "flags": set_ends((jax.random.randint(key_of[3], (NX, NY, NZ), 0, 3) < 1).astype(jnp.int32), jax.random.fold_in(key_of[3], 1), 0, 1),
        "mask_bits": draw_mask_bits(jax.random.fold_in(key_of[5], 71), 0),
    }


fictive_mass = 64.0
epsilon = 1e-06

def neighbour_table():
    table = []
    for across in range(-3, 4):
        for along in range(-3, 4):
            for upward in range(-3, 4):
                length = across * across + along * along + upward * upward
                if 0 < length <= 9:
                    table.append((across, along, upward))
    return table

def bond_forces(field_pad, words, words_pad, exist_pad):
    rows = words.shape[1]
    cols = words.shape[2]
    depth = words.shape[3]
    centre = field_pad[:, 3:3 + rows, 3:3 + cols, 3:3 + depth]
    totals = [jnp.zeros((rows, cols, depth), jnp.float32) for index in range(3)]
    for number, offset in enumerate(neighbour_table()):
        across, along, upward = offset
        word, bit = divmod(number, 31)
        mirror_word, mirror_bit = divmod(121 - number, 31)
        window = (slice(3 + across, 3 + across + rows), slice(3 + along, 3 + along + cols), slice(3 + upward, 3 + upward + depth))
        other = field_pad[(slice(None),) + window]
        own_flag = words[word] >> bit & 1
        far_flag = words_pad[mirror_word][window] >> mirror_bit & 1
        intact = (own_flag | far_flag == 0) & (exist_pad[window] > 0)
        length = float(across * across + along * along + upward * upward)
        weight = 1.0 / (length * math.sqrt(length))
        stretch = float(across) * (other[0] - centre[0]) + float(along) * (other[1] - centre[1]) + float(upward) * (other[2] - centre[2])
        scaled = jnp.where(intact, stretch * weight, jnp.float32(0.0))
        totals[0] = totals[0] + float(across) * scaled
        totals[1] = totals[1] + float(along) * scaled
        totals[2] = totals[2] + float(upward) * scaled
    return jnp.stack(totals)

def reference(disp, vel, load, flags, mask_bits):
    words_pad = jnp.pad(mask_bits, ((0, 0), (3, 3), (3, 3), (3, 3)))
    exist_pad = jnp.pad(jnp.ones(mask_bits.shape[1:], jnp.int32), 3)
    applied = flags.astype(jnp.float32)[None] * load
    count = 3.0 * NX * NY * NZ

    def internal(field):
        field_pad = jnp.pad(field, ((0, 0), (3, 3), (3, 3), (3, 3)))
        return bond_forces(field_pad, mask_bits, words_pad, exist_pad)
    previous = lax.fori_loop(0, 1, lambda index, carry: internal(disp - vel), jnp.zeros_like(disp))

    def relax(index, state):
        field, speed, before = state
        current = internal(field)
        total = current + applied
        kinetic = jnp.sum(speed * speed)
        rayleigh = jnp.sum(speed * (before - current))
        damping = 2.0 * jnp.sqrt(rayleigh / count / (fictive_mass * (kinetic / count + epsilon)))
        alpha = (2.0 - damping) / (2.0 + damping)
        beta = 2.0 / (fictive_mass * (2.0 + damping))
        speed = alpha * speed + beta * total
        return (field + speed, speed, current)
    field, speed, before = lax.fori_loop(0, ITERS, relax, (disp, vel, previous))
    return (field, speed)
```

```python
import functools
import math

import jax
import jax.numpy as jnp
from jax import lax
from jax.experimental import pallas as pl
from jax.experimental.pallas import tpu as pltpu
from jax.sharding import PartitionSpec as P

ITERS = 8
MESH = pl.DeviceIdType.MESH

fictive_mass = 64.0
epsilon = 1e-06

EDGE = 8


def neighbour_table():
    table = []
    for across in range(-3, 4):
        for along in range(-3, 4):
            for upward in range(-3, 4):
                length = across * across + along * along + upward * upward
                if 0 < length <= 9:
                    table.append((across, along, upward))
    return table


TABLE = neighbour_table()
NUMBER = {offset: number for number, offset in enumerate(TABLE)}


def reach(along, upward):
    return [a for a in range(-3, 4) if (a, along, upward) in NUMBER]


def rolled(cells, upward):
    depth = cells.shape[-1]
    if upward == 0:
        return cells
    return pltpu.roll(cells, (-upward) % depth, cells.ndim - 1)


def kernel(
    nx, ny,
    disp, vel, load, flags, mask,
    field, speed,
    weights, diagonal, pad, mask_pad, shifted, mask_shifted, mixed, plain, force, total, change,
    rim_x, rim_y, rim_c, pack_y, pack_c,
    mrim_x, mrim_y, mrim_c, mpack_y, mpack_c,
    sums_out, sums_in,
    send_sem, recv_sem, msend_sem, mrecv_sem, sum_send_sem, sum_recv_sem,
):
    rows, cols, depth = flags.shape
    count = 3.0 * rows * nx * cols * ny * depth
    devices = nx * ny
    my_x = lax.axis_index("gx")
    my_y = lax.axis_index("gy")

    sides = []
    for step_x, step_y in ((-1, 0), (1, 0), (0, -1), (0, 1), (-1, -1), (-1, 1), (1, -1), (1, 1)):
        there = None
        for step, mine, size in ((step_x, my_x, nx), (step_y, my_y, ny)):
            if step:
                near = mine > 0 if step < 0 else mine < size - 1
                there = near if there is None else there & near
        sides.append((step_x, step_y, there))

    def copies(index, source, rims, packs, sems, slot):
        step_x, step_y, there = sides[index]
        target = (my_x + step_x, my_y + step_y)
        if index < 2:
            start = 0 if step_x < 0 else rows - 3
            src = source.at[:, pl.ds(start, 3)]
            dst = rims[0].at[slot, 1 - index]
        elif index < 4:
            src = packs[0].at[slot, index - 2]
            dst = rims[1].at[slot, 3 - index]
        else:
            src = packs[1].at[slot, index - 4]
            dst = rims[2].at[slot, 7 - index]
        return pltpu.make_async_remote_copy(
            src_ref=src, dst_ref=dst,
            send_sem=sems[0].at[slot, index], recv_sem=sems[1].at[slot, index ^ 1 if index < 4 else 11 - index],
            device_id=target, device_id_type=MESH,
        )

    def exchange(source, rims, packs, sems, slot):
        for index in (0, 1):
            @pl.when(sides[index][2])
            def _():
                copies(index, source, rims, packs, sems, slot).start()
        parts = source.shape[0]
        for c in range(parts):
            for j in range(3):
                packs[0][slot, 0, c, j] = source[c, :, j, :]
                packs[0][slot, 1, c, j] = source[c, :, cols - 3 + j, :]
            for corner in range(4):
                step_x, step_y, _ = sides[4 + corner]
                for i in range(2):
                    x = i if step_x < 0 else rows - 2 + i
                    y = 0 if step_y < 0 else cols - 2
                    packs[1][slot, corner, c, pl.ds(2 * i, 2), :] = source[c, x, pl.ds(y, 2), :]
        for index in range(2, 8):
            @pl.when(sides[index][2])
            def _():
                copies(index, source, rims, packs, sems, slot).start()

    def arrive(source, rims, packs, sems, slot, padded):
        parts = source.shape[0]
        for index in range(8):
            step_x, step_y, there = sides[index]

            @pl.when(there)
            def _():
                step = copies(index, source, rims, packs, sems, slot)
                step.wait_send()
                back = copies(index ^ 1 if index < 4 else 11 - index, source, rims, packs, sems, slot)
                back.wait_recv()
                if index < 2:
                    first = 0 if step_x < 0 else 3 + rows
                    padded[:, pl.ds(first, 3), pl.ds(EDGE, cols), :] = rims[0][slot, index]
                elif index < 4:
                    first = EDGE - 3 if step_y < 0 else EDGE + cols
                    for c in range(parts):
                        for j in range(3):
                            padded[c, pl.ds(3, rows), first + j, :] = rims[1][slot, index - 2, c, j]
                else:
                    x = 1 if step_x < 0 else 3 + rows
                    y = EDGE - 2 if step_y < 0 else EDGE + cols
                    for c in range(parts):
                        for i in range(2):
                            padded[c, x + i, pl.ds(y, 2), :] = rims[2][slot, index - 4, c, pl.ds(2 * i, 2), :]

    rims, packs, sems = (rim_x, rim_y, rim_c), (pack_y, pack_c), (send_sem, recv_sem)
    mrims, mpacks, msems = (mrim_x, mrim_y, mrim_c), (mpack_y, mpack_c), (msend_sem, mrecv_sem)

    exchange(mask, mrims, mpacks, msems, 0)
    exchange(vel, rims, packs, sems, 0)
    exchange(disp, rims, packs, sems, 1)

    pad[...] = jnp.zeros_like(pad)
    mask_pad[...] = jnp.full_like(mask_pad, -1)
    mask_pad[:, pl.ds(3, rows), pl.ds(EDGE, cols), :] = mask[...]
    field[...] = disp[...]
    speed[...] = vel[...]
    diagonal[...] = jnp.zeros_like(diagonal)
    arrive(mask, mrims, mpacks, msems, 0, mask_pad)

    place = lax.broadcasted_iota(jnp.int32, (1, 1, depth), 2)
    for along in range(-3, 4):
        for word in range(4):
            mask_shifted[word] = mask_pad[word, :, pl.ds(EDGE + along, cols), :]
        for upward in range(-3, 4):
            across_all = reach(along, upward)
            if not across_all:
                continue
            inside = (place + upward >= 0) & (place + upward < depth)
            for low in range(0, rows, 4):
                moments = [None, None, None]
                for across in across_all:
                    number = NUMBER[(across, along, upward)]
                    word, bit = divmod(number, 31)
                    mirror_word, mirror_bit = divmod(121 - number, 31)
                    length = float(across * across + along * along + upward * upward)
                    weight = 1.0 / (length * math.sqrt(length))
                    own = mask[word, pl.ds(low, 4)] & (1 << bit)
                    far = mask_shifted[mirror_word, pl.ds(3 + low + across, 4)] & (1 << mirror_bit)
                    far = rolled(jnp.where(far == 0, jnp.float32(weight), jnp.float32(0.0)), upward)
                    one = jnp.where((own == 0) & inside, far, jnp.float32(0.0))
                    weights[number, pl.ds(low, 4)] = one
                    for power in range(3):
                        scale = float(across**power)
                        if scale != 0.0:
                            term = one if scale == 1.0 else scale * one
                            moments[power] = term if moments[power] is None else moments[power] + term
                for slot, (power, scale) in enumerate((
                    (2, 1), (1, along), (1, upward), (0, along * along), (0, along * upward), (0, upward * upward),
                )):
                    if scale and moments[power] is not None:
                        diagonal[slot, pl.ds(low, 4)] += float(scale) * moments[power]

    def apply_forces():
        for low in range(0, rows, 4):
            here = pl.ds(low, 4)
            u = [pad[c, pl.ds(3 + low, 4), pl.ds(EDGE, cols), :] for c in range(3)]
            d = [diagonal[slot, here] for slot in range(6)]
            force[0, here] = -(d[0] * u[0] + d[1] * u[1] + d[2] * u[2])
            force[1, here] = -(d[1] * u[0] + d[3] * u[1] + d[4] * u[2])
            force[2, here] = -(d[2] * u[0] + d[4] * u[1] + d[5] * u[2])
        turn = 0
        for along in range(-3, 4):
            for c in range(3):
                shifted[c] = pad[c, :, pl.ds(EDGE + along, cols), :]
            for upward in range(-3, 4):
                across_all = reach(along, upward)
                if not across_all:
                    continue
                turn = 1 - turn
                most = max(across_all)
                span = pl.ds(3 - most, rows + 2 * most)
                if along or upward:
                    mix = None
                    for scale, c in ((along, 1), (upward, 2)):
                        if scale:
                            term = float(scale) * shifted[c, span] if scale != 1 else shifted[c, span]
                            mix = term if mix is None else mix + term
                    mixed[turn, span] = rolled(mix, upward)
                if most:
                    plain[turn, span] = rolled(shifted[0, span], upward)
                for low in range(0, rows, 4):
                    here = pl.ds(low, 4)
                    whole = None
                    lean = None

                    def stretch(across):
                        at = pl.ds(3 + low + across, 4)
                        value = mixed[turn, at] if along or upward else None
                        if across:
                            term = float(across) * plain[turn, at]
                            value = term if value is None else value + term
                        return weights[NUMBER[(across, along, upward)], here] * value

                    for across in [a for a in across_all if a >= 0]:
                        if across == 0:
                            whole = stretch(0)
                            continue
                        up, down = stretch(across), stretch(-across)
                        both = up + down
                        whole = both if whole is None else whole + both
                        gap = float(across) * (up - down) if across != 1 else up - down
                        lean = gap if lean is None else lean + gap
                    if lean is not None:
                        force[0, here] += lean
                    if along:
                        force[1, here] += float(along) * whole
                    if upward:
                        force[2, here] += float(upward) * whole

    me = my_x * ny + my_y

    def send_sums(slot):
        kinetic = jnp.sum(speed[...] * speed[...], axis=(0, 1))
        rayleigh = jnp.sum(speed[...] * change[...], axis=(0, 1))
        sums_out[slot, pl.ds(0, 1), :] = jnp.sum(kinetic, axis=0, keepdims=True)
        sums_out[slot, pl.ds(1, 1), :] = jnp.sum(rayleigh, axis=0, keepdims=True)

        def send(r, carry):
            target = lax.rem(me + 1 + r, devices)
            pltpu.make_async_remote_copy(
                src_ref=sums_out.at[slot], dst_ref=sums_in.at[slot, r],
                send_sem=sum_send_sem.at[slot], recv_sem=sum_recv_sem.at[slot],
                device_id=(target // ny, lax.rem(target, ny)), device_id_type=MESH,
            ).start()
            return carry

        lax.fori_loop(0, devices - 1, send, 0)

    def take_sums(slot):
        whole = sums_in.at[slot]
        pltpu.make_async_copy(whole, whole, sum_send_sem.at[slot]).wait()
        pltpu.make_async_copy(whole, whole, sum_recv_sem.at[slot]).wait()
        both = jnp.sum(sums_in[slot], axis=0) + sums_out[slot]
        both = jnp.sum(both, axis=1, keepdims=True)
        kinetic = both[0:1]
        rayleigh = -both[1:2]
        damping = 2.0 * jnp.sqrt(rayleigh / count / (fictive_mass * (kinetic / count + epsilon)))
        alpha = (2.0 - damping) / (2.0 + damping)
        beta = 2.0 / (fictive_mass * (2.0 + damping))
        return alpha[None, None], beta[None, None]

    def advance(alpha, beta):
        for c in range(3):
            speed[c] = alpha[0] * speed[c] + beta[0] * total[c]
            field[c] = field[c] + speed[c]

    middle = (slice(None), pl.ds(3, rows), pl.ds(EDGE, cols), slice(None))

    def step(turn, carry):
        slot = jnp.where(turn < 2, turn, 2 + lax.rem(turn, 2))

        @pl.when(turn == 0)
        def _():
            pad[middle] = vel[...]

        @pl.when(turn == 1)
        def _():
            pad[middle] = disp[...]

        @pl.when(turn >= 2)
        def _():
            pad[middle] = total[...]

        arrive(total, rims, packs, sems, slot, pad)
        apply_forces()

        @pl.when(turn == 0)
        def _():
            change[...] = force[...]
            send_sums(0)

        @pl.when(turn == 1)
        def _():
            for c in range(3):
                total[c] = force[c] + flags[...].astype(jnp.float32) * load[c]
            exchange(total, rims, packs, sems, 2)

        @pl.when(turn >= 2)
        def _():
            alpha, beta = take_sums(lax.rem(turn, 2))
            advance(alpha, beta)
            for c in range(3):
                change[c] = alpha[0] * change[c] + beta[0] * force[c]
                total[c] = total[c] + change[c]

            @pl.when(turn < ITERS)
            def _():
                exchange(total, rims, packs, sems, 2 + lax.rem(turn + 1, 2))

            send_sums(lax.rem(turn + 1, 2))

        return carry

    lax.fori_loop(0, ITERS + 1, step, 0)
    alpha, beta = take_sums((ITERS + 1) % 2)
    advance(alpha, beta)


def on_device(nx, ny, disp, vel, load, flags, mask_bits):
    parts, rows, cols, depth = disp.shape
    words = mask_bits.shape[0]
    f32, i32 = jnp.float32, jnp.int32
    vmem, dma = pltpu.VMEM, pltpu.SemaphoreType.DMA
    wide = cols + 2 * EDGE
    block = (parts, rows, cols, depth)
    scratch = [
        vmem((len(TABLE), rows, cols, depth), f32),
        vmem((6, rows, cols, depth), f32),
        vmem((parts, rows + 6, wide, depth), f32),
        vmem((words, rows + 6, wide, depth), i32),
        vmem((parts, rows + 6, cols, depth), f32),
        vmem((words, rows + 6, cols, depth), i32),
        vmem((2, rows + 6, cols, depth), f32),
        vmem((2, rows + 6, cols, depth), f32),
        vmem(block, f32),
        vmem(block, f32),
        vmem(block, f32),
        vmem((4, 2, parts, 3, cols, depth), f32),
        vmem((4, 2, parts, 3, rows, depth), f32),
        vmem((4, 4, parts, 4, depth), f32),
        vmem((4, 2, parts, 3, rows, depth), f32),
        vmem((4, 4, parts, 4, depth), f32),
        vmem((1, 2, words, 3, cols, depth), i32),
        vmem((1, 2, words, 3, rows, depth), i32),
        vmem((1, 4, words, 4, depth), i32),
        vmem((1, 2, words, 3, rows, depth), i32),
        vmem((1, 4, words, 4, depth), i32),
        vmem((2, 2, depth), f32),
        vmem((2, nx * ny - 1, 2, depth), f32),
        dma((4, 8)),
        dma((4, 8)),
        dma((1, 8)),
        dma((1, 8)),
        dma((2,)),
        dma((2,)),
    ]
    return pl.pallas_call(
        functools.partial(kernel, nx, ny),
        out_shape=[jax.ShapeDtypeStruct(block, f32)] * 2,
        in_specs=[pl.BlockSpec(memory_space=vmem)] * 5,
        out_specs=[pl.BlockSpec(memory_space=vmem)] * 2,
        scratch_shapes=scratch,
        compiler_params=pltpu.CompilerParams(has_side_effects=True, vmem_limit_bytes=48 * 1024 * 1024),
    )(disp, vel, load, flags, mask_bits)


def solution(mesh):
    cells = P(None, "gx", "gy", None)
    return jax.shard_map(
        functools.partial(on_device, mesh.shape["gx"], mesh.shape["gy"]),
        mesh=mesh,
        in_specs=(cells, cells, cells, P("gx", "gy", None), cells),
        out_specs=(cells, cells),
        check_vma=False,
    )
```
